256 devices in a mesh: gz: 32 (over y, z), gy: 4 (over x), gx: 2 (over core).
Axes of the slice: x: 4, y: 4, z: 8, core: 2. Of those that a mesh axis runs over, the one named last changes fastest.
Arguments:
- right_side: float32 [256, 64, 256], P('gz', 'gy', 'gx'), may hold values from -128 to 128
- diagonal: float32 [256, 64, 256], P('gz', 'gy', 'gx'), may hold values from 0.05 to 1
Outputs:
- solution_field: float32 [256, 64, 256], P('gz', 'gy', 'gx')
- residual: float32 [256, 64, 256], P('gz', 'gy', 'gx')
The draws below stay inside these ranges and needn't reach their ends.
All inputs are finite; a program needn't handle non-finite values.
Results may differ from the reference program's by a relative error of at most 0.03.
Values sent between devices are 32-bit elements.
A program may use at most 64 MiB of HBM per device.

```python
import jax
import jax.numpy as jnp
import numpy as np
from jax import lax

S = 6
OUTER = 5
NZ = 256
NY = 64
NX = 256


def shard_levels(own_key, dims, pieces, low, largest):
    factor_of = 1.0
    for position, blocks in pieces:
        steps = jax.random.uniform(jax.random.fold_in(jax.random.fold_in(own_key, 6), position), (blocks,), jnp.float32, low / len(pieces), largest / len(pieces))
        factor_of = factor_of * jnp.repeat(jnp.exp(steps), dims[position] // blocks).reshape((-1,) + (1,) * (len(dims) - 1 - position))
    return factor_of


def gaussian(own_key, extent, spread, most, split=(), kind=jnp.bfloat16):
    result = spread * jax.random.normal(own_key, extent, jnp.float32)
    if split:
        result = result * shard_levels(own_key, extent, split, -0.22, 0.18)
    return jnp.clip(result, -most, most).astype(kind)


def setup_inputs(seed: int = 0) -> dict:
    key_list = jax.random.split(jax.random.key(seed), 3)
    return {
        "right_side": gaussian(key_list[0], (NZ, NY, NX), 24.0, 128.0, ((0, 32), (1, 4), (2, 2)), jnp.float32),
        "diagonal": jnp.clip(0.05 + 0.95 * jax.random.uniform(key_list[1], (NZ, NY, NX), jnp.float32) ** shard_levels(key_list[1], (NZ, NY, NX), ((0, 32), (1, 4), (2, 2)), -0.2, 0.2), 0.05, 1.0),
    }


center_shift = 19.0
half_width = 19.0


def apply_operator(padded, diagonal):
    extent_z = padded.shape[-3] - 2
    extent_y = padded.shape[-2] - 2
    extent_x = padded.shape[-1] - 2
    running = jnp.zeros(padded[..., 1:-1, 1:-1, 1:-1].shape, jnp.float32)
    for along_z in range(3):
        for along_y in range(3):
            for along_x in range(3):
                if along_z == 1 and along_y == 1 and along_x == 1:
                    continue
                running = running + padded[..., along_z:along_z + extent_z, along_y:along_y + extent_y, along_x:along_x + extent_x]
    return (26.0 + diagonal) * padded[..., 1:-1, 1:-1, 1:-1] - running


def chebyshev_next(images, current, previous):
    scaled = (images - center_shift * current) / half_width
    if previous is None:
        return scaled
    return 2.0 * scaled - previous


def basis_change():
    columns = 2 * S + 1
    matrix = np.zeros((columns, columns), np.float32)
    for offset, length in ((0, S), (S + 1, S - 1)):
        for degree in range(length):
            matrix[offset + degree, offset + degree] = center_shift
            if degree == 0:
                matrix[offset + 1, offset] = half_width
            else:
                matrix[offset + degree + 1, offset + degree] = 0.5 * half_width
                matrix[offset + degree - 1, offset + degree] = 0.5 * half_width
    return matrix


def coefficients(gram_matrix):
    columns = 2 * S + 1
    change = jnp.asarray(basis_change(), dtype=jnp.float32)
    identity = jnp.eye(columns, dtype=jnp.float32)
    dir_coeff = identity[0]
    res_coeff = identity[S + 1]
    sol_coeff = jnp.zeros((columns,), jnp.float32)
    for degree in range(S):
        moved = jnp.dot(change, dir_coeff, precision=lax.Precision.HIGHEST)
        norm_now = jnp.dot(res_coeff, jnp.dot(gram_matrix, res_coeff, precision=lax.Precision.HIGHEST), precision=lax.Precision.HIGHEST)
        curvature = jnp.dot(dir_coeff, jnp.dot(gram_matrix, moved, precision=lax.Precision.HIGHEST), precision=lax.Precision.HIGHEST)
        step_len = norm_now / curvature
        sol_coeff = sol_coeff + step_len * dir_coeff
        res_next = res_coeff - step_len * moved
        norm_next = jnp.dot(res_next, jnp.dot(gram_matrix, res_next, precision=lax.Precision.HIGHEST), precision=lax.Precision.HIGHEST)
        dir_coeff = res_next + (norm_next / norm_now) * dir_coeff
        res_coeff = res_next
    return sol_coeff, res_coeff, dir_coeff


def combine(coeff, basis_set):
    return jnp.tensordot(coeff, basis_set, axes=1, precision=lax.Precision.HIGHEST)


def reference(right_side, diagonal):
    solution = jnp.zeros(right_side.shape, jnp.float32)
    residual = right_side
    direction = right_side
    for outer_step in range(OUTER):
        p_fields = [direction]
        for degree in range(S):
            images = apply_operator(jnp.pad(p_fields[-1], 1), diagonal)
            p_fields.append(chebyshev_next(images, p_fields[-1], p_fields[-2] if degree else None))
        r_fields = [residual]
        for degree in range(S - 1):
            images = apply_operator(jnp.pad(r_fields[-1], 1), diagonal)
            r_fields.append(chebyshev_next(images, r_fields[-1], r_fields[-2] if degree else None))
        basis_set = jnp.stack(p_fields + r_fields)
        flattened = basis_set.reshape(basis_set.shape[0], -1)
        gram_matrix = jnp.dot(flattened, flattened.T, precision=lax.Precision.HIGHEST)
        sol_coeff, res_coeff, dir_coeff = coefficients(gram_matrix)
        solution = solution + combine(sol_coeff, basis_set)
        residual = combine(res_coeff, basis_set)
        direction = combine(dir_coeff, basis_set)
    return solution, residual
```

```python
import jax
import jax.numpy as jnp
from jax import lax
from jax.experimental import pallas as pl
from jax.experimental.pallas import tpu as pltpu
from jax.sharding import PartitionSpec as P

S = 6
OUTER = 5
ROUNDS = 3
DEG = S * OUTER // ROUNDS
HALO = DEG // 2
SHIFT = 19.0
HALF = 19.0
LANES = 128
ROWS = 8
BLOCK = 64
MESH = pl.DeviceIdType.MESH


def two_sum(a, b):
    s = a + b
    t = s - a
    return s, (a - (s - t)) + (b - t)


def pair_add(a, b):
    s, e = two_sum(a[0], b[0])
    e = e + (a[1] + b[1])
    h = s + e
    return h, e - (h - s)


def split(a):
    c = 4097.0 * a
    high = c - (c - a)
    return high, a - high


def pair_scale(a, b, b_parts):
    p = a[0] * b
    h, l = split(a[0])
    e = ((h * b_parts[0] - p) + h * b_parts[1] + l * b_parts[0]) + l * b_parts[1]
    e = e + a[1] * b
    s = p + e
    return s, e - (s - p)


def kernel(nz, ny, nx, rhs_ref, diag_ref, sol_out, res_out,
           fields, p_low, r_low, p_wave, r_wave, p_high, r_high, scale2, weight, total, pairs,
           a_send, a_recv, b_send, b_recv, final,
           z_send, z_recv, y_send, y_recv, a_ssem, a_rsem, b_ssem, b_rsem, swap_send, swap_recv, own_sem):
    bz, by, bx = rhs_ref.shape
    hy = by // 2
    ze, halves, ya = fields.shape[1:4]
    first = (ya - hy) // 2
    low_rows, high_rows = slice(first - ROWS, first), slice(first + hy, first + hy + ROWS)
    iz, iy, ix = lax.axis_index("gz"), lax.axis_index("gy"), lax.axis_index("gx")
    other = 1 - ix
    yy = iy * 2 + ix
    has_z = (iz > 0, iz < nz - 1)
    has_y = (yy > 0, yy < 2 * ny - 1)
    z_dev = tuple((iz + s, iy, ix) for s in (-1, 1))
    y_dev = tuple((iz, (yy + s) // 2, other) for s in (-1, 1))
    mid_z, mid_y = slice(HALO, HALO + bz), slice(first, first + hy)
    RES, DIR, DIA, DIR5, RES5 = range(5)

    def row_tile(index):
        return pl.ds(pl.multiple_of(index * hy, hy), hy)

    swaps, owns = [], []
    for k, (ref, field) in enumerate(((rhs_ref, DIR), (diag_ref, DIA))):
        spot = fields.at[field, mid_z, ix, mid_y, :]
        swap = pltpu.make_async_remote_copy(
            src_ref=ref.at[:, row_tile(other), :], dst_ref=spot,
            send_sem=swap_send.at[k], recv_sem=swap_recv.at[k],
            device_id=(iz, iy, other), device_id_type=MESH)
        swap.start()
        own = pltpu.make_async_copy(ref.at[:, row_tile(ix), :], spot, own_sem.at[k])
        own.start()
        swaps.append(swap)
        owns.append(own)

    for side in range(2):
        planes = slice(0, HALO) if side == 0 else slice(HALO + bz, ze)
        rows = (low_rows, high_rows)[side]

        @pl.when(jnp.logical_not(has_z[side]))
        def _():
            for k in range(5):
                fields[k, planes] = jnp.zeros((HALO, halves, ya, bx), jnp.float32)

        @pl.when(jnp.logical_not(has_y[side]))
        def _():
            for k in range(5):
                fields[k, :, :, rows, :] = jnp.zeros((ze, halves, ROWS, bx), jnp.float32)

    w_unit = 2.0 / HALF
    w_low = jnp.where(has_y[0], jnp.float32(w_unit), 0.0)
    w_high = jnp.where(has_y[1], jnp.float32(w_unit), 0.0)
    z_low = jnp.where(has_z[0], jnp.float32(1.0), 0.0)
    z_high = jnp.where(has_z[1], jnp.float32(1.0), 0.0)
    for plane in range(ze):
        factor = z_low if plane < HALO else (z_high if plane >= HALO + bz else jnp.float32(1.0))
        for tile, w in enumerate((w_low, jnp.float32(w_unit), w_high)):
            weight[plane, tile] = jnp.broadcast_to(w * factor, (ROWS, bx))
    total[...] = jnp.zeros(total.shape, jnp.float32)
    pairs[...] = jnp.zeros(pairs.shape, jnp.float32)

    for copy in owns + swaps:
        copy.wait()

    def z_copy(item, side):
        field, depth, k = item
        low_src, high_src = slice(HALO, HALO + depth), slice(HALO + bz - depth, HALO + bz)
        low_dst, high_dst = slice(HALO - depth, HALO), slice(HALO + bz, HALO + bz + depth)
        src, dst = ((low_src, high_dst), (high_src, low_dst))[side]
        return pltpu.make_async_remote_copy(
            src_ref=fields.at[field, src, :, mid_y, :], dst_ref=fields.at[field, dst, :, mid_y, :],
            send_sem=z_send.at[k, side], recv_sem=z_recv.at[k, 1 - side],
            device_id=z_dev[side], device_id_type=MESH)

    def y_copy(item, side, part):
        field, depth, k = item
        planes = (mid_z, slice(HALO - depth, HALO), slice(HALO + bz, HALO + bz + depth))[part]
        low_src, high_src = slice(first, first + depth), slice(first + hy - depth, first + hy)
        low_dst, high_dst = slice(first - depth, first), slice(first + hy, first + hy + depth)
        src, dst = ((low_src, high_dst), (high_src, low_dst))[side]
        return pltpu.make_async_remote_copy(
            src_ref=fields.at[field, planes, :, src, :], dst_ref=fields.at[field, planes, :, dst, :],
            send_sem=y_send.at[k, side, part], recv_sem=y_recv.at[k, 1 - side, part],
            device_id=y_dev[side], device_id_type=MESH)

    def exchange(items):
        for item in items:
            for side in range(2):
                @pl.when(has_z[side])
                def _():
                    z_copy(item, side).start()
        for item in items:
            for side in range(2):
                @pl.when(has_y[side])
                def _():
                    y_copy(item, side, 0).start()
        for item in items:
            for z_side in range(2):
                @pl.when(has_z[z_side])
                def _():
                    z_copy(item, 1 - z_side).wait_recv()
                    for side in range(2):
                        @pl.when(has_y[side])
                        def _():
                            y_copy(item, side, 1 + z_side).start()
        for item in items:
            for side in range(2):
                @pl.when(has_z[side])
                def _():
                    z_copy(item, side).wait_send()

                @pl.when(has_y[side])
                def _():
                    y_copy(item, side, 0).wait_send()
                    y_copy(item, 1 - side, 0).wait_recv()
                    for z_side in range(2):
                        @pl.when(has_z[z_side])
                        def _():
                            y_copy(item, side, 1 + z_side).wait_send()
                            y_copy(item, 1 - side, 1 + z_side).wait_recv()

    exchange(((DIR, HALO, 0), (DIA, HALO - 1, 1)))
    all_rows = slice(first - ROWS, first + hy + ROWS)

    def prepare(plane, c):
        scale2[plane] = (fields[DIA, plane, :, all_rows, :] + (27.0 - SHIFT)) * (2.0 / HALF)
        return c
    lax.fori_loop(0, ze, prepare, 0)

    tiles = (hy + 2 * ROWS) // ROWS
    lane_id = lax.broadcasted_iota(jnp.int32, (ROWS, bx), 1)
    first_lane, last_lane = lane_id == 0, lane_id == bx - 1

    def row_sums(ref, z, tile):
        at = first - ROWS + tile * ROWS
        return [ref[z, h, at - 1:at - 1 + ROWS, :] + ref[z, h, at:at + ROWS, :] + ref[z, h, at + 1:at + 1 + ROWS, :]
                for h in range(halves)]

    def lane_sums(parts):
        left = [pltpu.roll(v, 1, 1) for v in parts]
        right = [pltpu.roll(v, bx - 1, 1) for v in parts]
        out = []
        for h in range(halves):
            before = left[h - 1] if h else 0.0
            after = right[h + 1] if h < halves - 1 else 0.0
            out.append(parts[h] + jnp.where(first_lane, before, left[h]) + jnp.where(last_lane, after, right[h]))
        return out

    p_at = [fields.at[DIR]] + [p_low.at[k] for k in range(HALO - 1)] + [fields.at[DIR5]]
    r_at = [fields.at[RES]] + [r_low.at[k] for k in range(HALO - 1)] + [fields.at[RES5]]
    p_on = [fields.at[DIR5]] + [p_wave.at[k] for k in range(HALO)]
    r_on = [fields.at[RES5]] + [r_wave.at[k] for k in range(HALO - 1)]

    def sweep(chain, degree, depth):
        start, stop = HALO - depth, HALO + bz + depth
        chosen = range(tiles) if depth else (1,)

        def step(z, carry):
            out = []
            for tile, (before, here) in zip(chosen, carry):
                after = row_sums(chain[degree], z + 1, tile)
                box = lane_sums([a + b + c for a, b, c in zip(before, here, after)])
                at = first - ROWS + tile * ROWS
                for h in range(halves):
                    value = (scale2[z, h, tile * ROWS:(tile + 1) * ROWS, :] * chain[degree][z, h, at:at + ROWS, :]
                             - weight[z, tile] * box[h])
                    if degree == 0:
                        value = 0.5 * value
                    else:
                        value = value - chain[degree - 1][z, h, at:at + ROWS, :]
                    chain[degree + 1][z, h, at:at + ROWS, :] = value
                out.append((here, after))
            return tuple(out)
        carry = tuple((row_sums(chain[degree], start - 1, k), row_sums(chain[degree], start, k)) for k in chosen)
        for z in range(start, stop):
            carry = step(z, carry)

    gl = lax.broadcasted_iota(jnp.int32, (ROWS, LANES), 1)
    zero_lane, up_twice = gl == 0, jnp.where((gl == 1) | (gl == BLOCK + 1), jnp.float32(2.0), jnp.float32(1.0))
    in_block = (gl <= DEG) | ((gl >= BLOCK) & (gl <= BLOCK + DEG))

    def pick(v, lane):
        return jnp.broadcast_to(v[:, lane:lane + 1], (ROWS, LANES))

    def moved(pair):
        up = [pltpu.roll(v, LANES - 1, 1) for v in pair]
        down = [jnp.where(zero_lane, u, pltpu.roll(v, 1, 1)) for u, v in zip(up, pair)]
        return pair_add((2.0 * pair[0], 2.0 * pair[1]), pair_add(up, down))

    def apply_b(c):
        return jnp.where(in_block, 2.0 * c + up_twice * pltpu.roll(c, 1, 1) + pltpu.roll(c, LANES - 1, 1), 0.0)

    def everywhere(row, slot):
        a_me, b_me = yy, iz
        a_count, b_count = ny * nx, nz

        def stage(send_ref, recv_ref, me, count, ssem, rsem, dev, value):
            send_ref[...] = value
            recv_ref[slot, me] = value
            for k in range(1, count):
                peer = (me + k) % count
                pltpu.make_async_remote_copy(
                    src_ref=send_ref, dst_ref=recv_ref.at[slot, me],
                    send_sem=ssem, recv_sem=rsem.at[slot],
                    device_id=dev(peer), device_id_type=MESH).start()
            most = recv_ref.at[slot, 0:count - 1]
            pltpu.make_async_copy(most, most, rsem.at[slot]).wait()
            out = jnp.sum(recv_ref[slot], axis=0)
            pltpu.make_async_copy(most, most, ssem).wait()
            return out
        mine = stage(a_send, a_recv, a_me, a_count, a_ssem, a_rsem, lambda p: (iz, p // nx, p % nx), row)
        return stage(b_send, b_recv, b_me, b_count, b_ssem, b_rsem, lambda p: (p, iy, ix), mine)

    def outer(t, two):
        for degree in range(HALO):
            sweep(p_at, degree, HALO - 1 - degree)
            if two:
                sweep(r_at, degree, HALO - 1 - degree)
        exchange(((DIR5, HALO, 2), (RES5, HALO - 1, 3)) if two else ((DIR5, HALO, 2),))
        for degree in range(HALO):
            sweep(p_on, degree, HALO - 1 - degree)
            if two and degree < HALO - 1:
                sweep(r_on, degree, HALO - 2 - degree)

        sums = {}

        def add(key, value):
            sums[key] = sums[key] + value if key in sums else value
        for z in range(bz):
            for h in range(halves):
                here = (HALO + z, h, mid_y, slice(None))
                lists = []
                for low, wave, high in ((p_at, p_on, p_high), (r_at, r_on, r_high))[:1 + two]:
                    vs = [ref[here] for ref in low]
                    for k in range(1, len(wave)):
                        value = 2.0 * wave[k][here] - vs[HALO - k]
                        high[k - 1, z, h] = value
                        vs.append(value)
                    lists.append(vs)
                ps = lists[0]
                for k in range(2 * DEG + 1):
                    add(k, ps[(k + 1) // 2] * ps[k // 2])
                if two:
                    rs = lists[1]
                    for k in range(2 * DEG):
                        add(BLOCK + k, ps[(k + 1) // 2] * rs[k // 2])
        lines = {}
        for key, value in sums.items():
            base = key // BLOCK * BLOCK
            if key - base > 1:
                value = 2.0 * value - sums[base + (key - base) % 2]
            pairs[key:key + 1, :] = jnp.sum(value, axis=0, keepdims=True)
        row = jnp.sum(pairs[...].T, axis=0, keepdims=True)
        row = jnp.broadcast_to(everywhere(row, t), (ROWS, LANES))

        nil = jnp.zeros((ROWS, LANES), jnp.float32)
        pi = (row, nil)
        rho = (pltpu.roll(row, LANES - BLOCK, 1), nil) if two else pi
        p_c = (gl == 0).astype(jnp.float32)
        r_c = (gl == BLOCK).astype(jnp.float32) if two else p_c
        x_c = nil
        rho_k = pick(rho[0], 0)
        for k in range(DEG):
            q = moved(pi)
            length = rho_k / pick(q[0], k)
            less = -length
            change = pair_scale(q, less, split(less))
            rho = pair_add(rho, change)
            fresh = pick(rho[0], k + 1)
            ratio = (-2.0 if k == 0 else -1.0) * length * (fresh / rho_k)
            pi = pair_add(rho, pair_scale(pi, ratio, split(ratio)))
            rho_k = fresh
            q_c = apply_b(p_c)
            x_c = x_c + (length * (2.0 / HALF)) * p_c
            r_c = r_c - length * q_c
            p_c = r_c + ratio * p_c

        lanes = list(range(DEG + 1)) + (list(range(BLOCK, BLOCK + DEG)) if two else [])
        xw, rw, pw = ([pick(c, lane) for lane in lanes] for c in (x_c, r_c, p_c))
        for z in range(bz):
            for h in range(halves):
                here = (HALO + z, h, mid_y, slice(None))
                vs = [ref[here] for ref in p_at] + [p_high[k, z, h] for k in range(HALO)]
                if two:
                    vs += [ref[here] for ref in r_at] + [r_high[k, z, h] for k in range(HALO - 1)]

                def mix(w):
                    out = w[0] * vs[0]
                    for a, b in zip(w[1:], vs[1:]):
                        out = out + a * b
                    return out
                total[0, z, h] = total[0, z, h] + mix(xw)
                fields[RES, HALO + z, h, mid_y, :] = mix(rw)
                fields[DIR, HALO + z, h, mid_y, :] = mix(pw)

    outer(0, False)

    def later(t, carry):
        exchange(((DIR, HALO, 0), (RES, HALO, 1)))
        outer(t, True)
        return carry
    lax.fori_loop(1, ROUNDS, later, 0)

    total[1] = fields[RES, mid_z, :, mid_y, :]
    back = pltpu.make_async_remote_copy(
        src_ref=total.at[:, :, other], dst_ref=final,
        send_sem=swap_send.at[0], recv_sem=swap_recv.at[0],
        device_id=(iz, iy, other), device_id_type=MESH)
    back.start()
    for k, out in enumerate((sol_out, res_out)):
        out[:, row_tile(ix), :] = total[k, :, ix]
    back.wait()
    for k, out in enumerate((sol_out, res_out)):
        out[:, row_tile(other), :] = final[k]


def solution(mesh):
    nz, ny, nx = mesh.shape["gz"], mesh.shape["gy"], mesh.shape["gx"]

    def body(right_side, diagonal):
        bz, by, bx = right_side.shape
        hy = by // 2
        assert nx == 2 and bz >= HALO and hy == ROWS and bx == LANES
        ze, ye = bz + 2 * HALO, hy + 4 * ROWS
        f32, dma = jnp.float32, pltpu.SemaphoreType.DMA
        return pl.pallas_call(
            lambda *refs: kernel(nz, ny, nx, *refs),
            out_shape=(jax.ShapeDtypeStruct(right_side.shape, f32),) * 2,
            in_specs=[pl.BlockSpec(memory_space=pltpu.VMEM)] * 2,
            out_specs=(pl.BlockSpec(memory_space=pltpu.VMEM),) * 2,
            scratch_shapes=[
                pltpu.VMEM((5, ze, nx, ye, bx), f32),
                pltpu.VMEM((HALO - 1, ze, nx, ye, bx), f32),
                pltpu.VMEM((HALO - 1, ze, nx, ye, bx), f32),
                pltpu.VMEM((HALO, ze, nx, ye, bx), f32),
                pltpu.VMEM((HALO - 1, ze, nx, ye, bx), f32),
                pltpu.VMEM((HALO, bz, nx, hy, bx), f32),
                pltpu.VMEM((HALO - 1, bz, nx, hy, bx), f32),
                pltpu.VMEM((ze, nx, hy + 2 * ROWS, bx), f32),
                pltpu.VMEM((ze, 3, ROWS, bx), f32),
                pltpu.VMEM((2, bz, nx, hy, bx), f32),
                pltpu.VMEM((LANES, LANES), f32),
                pltpu.VMEM((1, LANES), f32),
                pltpu.VMEM((ROUNDS, ny * nx, 1, LANES), f32),
                pltpu.VMEM((1, LANES), f32),
                pltpu.VMEM((ROUNDS, nz, 1, LANES), f32),
                pltpu.VMEM((2, bz, hy, bx), f32),
                dma((4, 2)), dma((4, 2)), dma((4, 2, 3)), dma((4, 2, 3)),
                dma, dma((ROUNDS,)), dma, dma((ROUNDS,)),
                dma((2,)), dma((2,)), dma((2,)),
            ],
            compiler_params=pltpu.CompilerParams(has_side_effects=True),
        )(right_side, diagonal)

    spec = P("gz", "gy", "gx")
    return jax.shard_map(body, mesh=mesh, in_specs=(spec, spec), out_specs=(spec, spec), check_vma=False)
```

```python
import jax
import jax.numpy as jnp
from jax import lax
from jax.experimental import pallas as pl
from jax.experimental.pallas import tpu as pltpu
from jax.sharding import PartitionSpec as P

S = 6
OUTER = 5
ROUNDS = 3
DEG = S * OUTER // ROUNDS
HALO = DEG // 2
SHIFT = 19.0
HALF = 19.0
LANES = 128
ROWS = 8
BLOCK = 64
MESH = pl.DeviceIdType.MESH


def two_sum(a, b):
    s = a + b
    t = s - a
    return s, (a - (s - t)) + (b - t)


def pair_add(a, b):
    s, e = two_sum(a[0], b[0])
    e = e + (a[1] + b[1])
    h = s + e
    return h, e - (h - s)


def split(a):
    c = 4097.0 * a
    high = c - (c - a)
    return high, a - high


def pair_scale(a, b, b_parts):
    p = a[0] * b
    h, l = split(a[0])
    e = ((h * b_parts[0] - p) + h * b_parts[1] + l * b_parts[0]) + l * b_parts[1]
    e = e + a[1] * b
    s = p + e
    return s, e - (s - p)


def kernel(nz, ny, nx, rhs_ref, diag_ref, sol_out, res_out,
           fields, p_low, r_low, p_wave, r_wave, p_high, r_high, scale2, weight, total, pairs,
           a_send, a_recv, b_send, b_recv,
           z_send, z_recv, y_send, y_recv, a_ssem, a_rsem, b_ssem, b_rsem, swap_send, swap_recv, own_sem):
    bz, by, bx = rhs_ref.shape
    hy = by // 2
    ze, halves, ya = fields.shape[1:4]
    first = (ya - hy) // 2
    low_rows, high_rows = slice(first - ROWS, first), slice(first + hy, first + hy + ROWS)
    iz, iy, ix = lax.axis_index("gz"), lax.axis_index("gy"), lax.axis_index("gx")
    other = 1 - ix
    yy = iy * 2 + ix
    has_z = (iz > 0, iz < nz - 1)
    has_y = (yy > 0, yy < 2 * ny - 1)
    z_dev = tuple((iz + s, iy, ix) for s in (-1, 1))
    y_dev = tuple((iz, (yy + s) // 2, other) for s in (-1, 1))
    mid_z, mid_y = slice(HALO, HALO + bz), slice(first, first + hy)
    RES, DIR, DIA, DIR5, RES5 = range(5)

    def row_tile(index):
        return pl.ds(pl.multiple_of(index * hy, hy), hy)

    barrier = pltpu.get_barrier_semaphore()
    for k in range(1, ny * nx):
        peer = (yy + k) % (ny * nx)
        pl.semaphore_signal(barrier, inc=1, device_id=(iz, peer // nx, peer % nx), device_id_type=MESH)
    for k in range(1, nz):
        pl.semaphore_signal(barrier, inc=1, device_id=((iz + k) % nz, iy, ix), device_id_type=MESH)

    owns = []
    spots = [(ref, fields.at[field, mid_z, ix, mid_y, :]) for ref, field in ((rhs_ref, DIR), (diag_ref, DIA))]
    for k, (ref, spot) in enumerate(spots):
        own = pltpu.make_async_copy(ref.at[:, row_tile(ix), :], spot, own_sem.at[k])
        own.start()
        owns.append(own)

    for side in range(2):
        planes = slice(0, HALO) if side == 0 else slice(HALO + bz, ze)
        rows = (low_rows, high_rows)[side]

        @pl.when(jnp.logical_not(has_z[side]))
        def _():
            for k in range(5):
                fields[k, planes] = jnp.zeros((HALO, halves, ya, bx), jnp.float32)

        @pl.when(jnp.logical_not(has_y[side]))
        def _():
            for k in range(5):
                fields[k, :, :, rows, :] = jnp.zeros((ze, halves, ROWS, bx), jnp.float32)

    w_unit = 2.0 / HALF
    w_low = jnp.where(has_y[0], jnp.float32(w_unit), 0.0)
    w_high = jnp.where(has_y[1], jnp.float32(w_unit), 0.0)
    z_low = jnp.where(has_z[0], jnp.float32(1.0), 0.0)
    z_high = jnp.where(has_z[1], jnp.float32(1.0), 0.0)
    for plane in range(ze):
        factor = z_low if plane < HALO else (z_high if plane >= HALO + bz else jnp.float32(1.0))
        for tile, w in enumerate((w_low, jnp.float32(w_unit), w_high)):
            weight[plane, tile] = jnp.broadcast_to(w * factor, (ROWS, bx))
    total[...] = jnp.zeros(total.shape, jnp.float32)
    pairs[...] = jnp.zeros(pairs.shape, jnp.float32)

    pl.semaphore_wait(barrier, ny * nx - 1 + nz - 1)
    swaps = []
    for k, (ref, spot) in enumerate(spots):
        swap = pltpu.make_async_remote_copy(
            src_ref=ref.at[:, row_tile(other), :], dst_ref=spot,
            send_sem=swap_send.at[k], recv_sem=swap_recv.at[k],
            device_id=(iz, iy, other), device_id_type=MESH)
        swap.start()
        swaps.append(swap)
    for copy in owns + swaps:
        copy.wait()

    def z_copy(item, side):
        field, depth, k = item
        low_src, high_src = slice(HALO, HALO + depth), slice(HALO + bz - depth, HALO + bz)
        low_dst, high_dst = slice(HALO - depth, HALO), slice(HALO + bz, HALO + bz + depth)
        src, dst = ((low_src, high_dst), (high_src, low_dst))[side]
        return pltpu.make_async_remote_copy(
            src_ref=fields.at[field, src, :, mid_y, :], dst_ref=fields.at[field, dst, :, mid_y, :],
            send_sem=z_send.at[k, side], recv_sem=z_recv.at[k, 1 - side],
            device_id=z_dev[side], device_id_type=MESH)

    def y_copy(item, side, part):
        field, depth, k = item
        planes = (mid_z, slice(HALO - depth, HALO), slice(HALO + bz, HALO + bz + depth))[part]
        low_src, high_src = slice(first, first + depth), slice(first + hy - depth, first + hy)
        low_dst, high_dst = slice(first - depth, first), slice(first + hy, first + hy + depth)
        src, dst = ((low_src, high_dst), (high_src, low_dst))[side]
        return pltpu.make_async_remote_copy(
            src_ref=fields.at[field, planes, :, src, :], dst_ref=fields.at[field, planes, :, dst, :],
            send_sem=y_send.at[k, side, part], recv_sem=y_recv.at[k, 1 - side, part],
            device_id=y_dev[side], device_id_type=MESH)

    def exchange(items):
        for item in items:
            for side in range(2):
                @pl.when(has_z[side])
                def _():
                    z_copy(item, side).start()
        for item in items:
            for side in range(2):
                @pl.when(has_y[side])
                def _():
                    y_copy(item, side, 0).start()
        for item in items:
            for z_side in range(2):
                @pl.when(has_z[z_side])
                def _():
                    z_copy(item, 1 - z_side).wait_recv()
                    for side in range(2):
                        @pl.when(has_y[side])
                        def _():
                            y_copy(item, side, 1 + z_side).start()
        for item in items:
            for side in range(2):
                @pl.when(has_z[side])
                def _():
                    z_copy(item, side).wait_send()

                @pl.when(has_y[side])
                def _():
                    y_copy(item, side, 0).wait_send()
                    y_copy(item, 1 - side, 0).wait_recv()
                    for z_side in range(2):
                        @pl.when(has_z[z_side])
                        def _():
                            y_copy(item, side, 1 + z_side).wait_send()
                            y_copy(item, 1 - side, 1 + z_side).wait_recv()

    exchange(((DIR, HALO, 0), (DIA, HALO - 1, 1)))
    all_rows = slice(first - ROWS, first + hy + ROWS)

    def prepare(plane, c):
        scale2[plane] = (fields[DIA, plane, :, all_rows, :] + (27.0 - SHIFT)) * (2.0 / HALF)
        return c
    lax.fori_loop(0, ze, prepare, 0)

    tiles = (hy + 2 * ROWS) // ROWS
    lane_id = lax.broadcasted_iota(jnp.int32, (ROWS, bx), 1)
    first_lane, last_lane = lane_id == 0, lane_id == bx - 1

    def row_sums(ref, z, tile):
        at = first - ROWS + tile * ROWS
        return [ref[z, h, at - 1:at - 1 + ROWS, :] + ref[z, h, at:at + ROWS, :] + ref[z, h, at + 1:at + 1 + ROWS, :]
                for h in range(halves)]

    def lane_sums(parts):
        left = [pltpu.roll(v, 1, 1) for v in parts]
        right = [pltpu.roll(v, bx - 1, 1) for v in parts]
        out = []
        for h in range(halves):
            before = left[h - 1] if h else 0.0
            after = right[h + 1] if h < halves - 1 else 0.0
            out.append(parts[h] + jnp.where(first_lane, before, left[h]) + jnp.where(last_lane, after, right[h]))
        return out

    p_at = [fields.at[DIR]] + [p_low.at[k] for k in range(HALO - 1)] + [fields.at[DIR5]]
    r_at = [fields.at[RES]] + [r_low.at[k] for k in range(HALO - 1)] + [fields.at[RES5]]
    p_on = [fields.at[DIR5]] + [p_wave.at[k] for k in range(HALO)]
    r_on = [fields.at[RES5]] + [r_wave.at[k] for k in range(HALO - 1)]

    def sweep(chain, degree, depth):
        start, stop = HALO - depth, HALO + bz + depth
        chosen = range(tiles) if depth else (1,)

        def step(z, carry):
            out = []
            for tile, (before, here) in zip(chosen, carry):
                after = row_sums(chain[degree], z + 1, tile)
                box = lane_sums([a + b + c for a, b, c in zip(before, here, after)])
                at = first - ROWS + tile * ROWS
                for h in range(halves):
                    value = (scale2[z, h, tile * ROWS:(tile + 1) * ROWS, :] * chain[degree][z, h, at:at + ROWS, :]
                             - weight[z, tile] * box[h])
                    if degree == 0:
                        value = 0.5 * value
                    else:
                        value = value - chain[degree - 1][z, h, at:at + ROWS, :]
                    chain[degree + 1][z, h, at:at + ROWS, :] = value
                out.append((here, after))
            return tuple(out)
        carry = tuple((row_sums(chain[degree], start - 1, k), row_sums(chain[degree], start, k)) for k in chosen)
        for z in range(start, stop):
            carry = step(z, carry)

    gl = lax.broadcasted_iota(jnp.int32, (ROWS, LANES), 1)
    zero_lane, up_twice = gl == 0, jnp.where((gl == 1) | (gl == BLOCK + 1), jnp.float32(2.0), jnp.float32(1.0))
    in_block = (gl <= DEG) | ((gl >= BLOCK) & (gl <= BLOCK + DEG))

    def pick(v, lane):
        return jnp.broadcast_to(v[:, lane:lane + 1], (ROWS, LANES))

    def moved(pair):
        up = [pltpu.roll(v, LANES - 1, 1) for v in pair]
        down = [jnp.where(zero_lane, u, pltpu.roll(v, 1, 1)) for u, v in zip(up, pair)]
        return pair_add((2.0 * pair[0], 2.0 * pair[1]), pair_add(up, down))

    def apply_b(c):
        return jnp.where(in_block, 2.0 * c + up_twice * pltpu.roll(c, 1, 1) + pltpu.roll(c, LANES - 1, 1), 0.0)

    def everywhere(row, slot):
        a_me, b_me = yy, iz
        a_count, b_count = ny * nx, nz

        def stage(send_ref, recv_ref, me, count, ssem, rsem, dev, value):
            send_ref[...] = value
            recv_ref[slot, me] = value
            for k in range(1, count):
                peer = (me + k) % count
                pltpu.make_async_remote_copy(
                    src_ref=send_ref, dst_ref=recv_ref.at[slot, me],
                    send_sem=ssem, recv_sem=rsem.at[slot],
                    device_id=dev(peer), device_id_type=MESH).start()
            most = recv_ref.at[slot, 0:count - 1]
            pltpu.make_async_copy(most, most, rsem.at[slot]).wait()
            out = jnp.sum(recv_ref[slot], axis=0)
            pltpu.make_async_copy(most, most, ssem).wait()
            return out
        mine = stage(a_send, a_recv, a_me, a_count, a_ssem, a_rsem, lambda p: (iz, p // nx, p % nx), row)
        return stage(b_send, b_recv, b_me, b_count, b_ssem, b_rsem, lambda p: (p, iy, ix), mine)

    def outer(t, two):
        for degree in range(HALO):
            sweep(p_at, degree, HALO - 1 - degree)
            if two:
                sweep(r_at, degree, HALO - 1 - degree)
        exchange(((DIR5, HALO, 2), (RES5, HALO - 1, 3)) if two else ((DIR5, HALO, 2),))
        for degree in range(HALO):
            sweep(p_on, degree, HALO - 1 - degree)
            if two and degree < HALO - 1:
                sweep(r_on, degree, HALO - 2 - degree)

        sums = {}

        def add(key, value):
            sums[key] = sums[key] + value if key in sums else value
        for z in range(bz):
            for h in range(halves):
                here = (HALO + z, h, mid_y, slice(None))
                lists = []
                for low, wave, high in ((p_at, p_on, p_high), (r_at, r_on, r_high))[:1 + two]:
                    vs = [ref[here] for ref in low]
                    for k in range(1, len(wave)):
                        value = 2.0 * wave[k][here] - vs[HALO - k]
                        high[k - 1, z, h] = value
                        vs.append(value)
                    lists.append(vs)
                ps = lists[0]
                for k in range(2 * DEG + 1):
                    add(k, ps[(k + 1) // 2] * ps[k // 2])
                if two:
                    rs = lists[1]
                    for k in range(2 * DEG):
                        add(BLOCK + k, ps[(k + 1) // 2] * rs[k // 2])
        lines = {}
        for key, value in sums.items():
            base = key // BLOCK * BLOCK
            if key - base > 1:
                value = 2.0 * value - sums[base + (key - base) % 2]
            pairs[key:key + 1, :] = jnp.sum(value, axis=0, keepdims=True)
        row = jnp.sum(pairs[...].T, axis=0, keepdims=True)
        row = jnp.broadcast_to(everywhere(row, t), (ROWS, LANES))

        nil = jnp.zeros((ROWS, LANES), jnp.float32)
        pi = (row, nil)
        rho = (pltpu.roll(row, LANES - BLOCK, 1), nil) if two else pi
        p_c = (gl == 0).astype(jnp.float32)
        r_c = (gl == BLOCK).astype(jnp.float32) if two else p_c
        x_c = nil
        rho_k = pick(rho[0], 0)
        for k in range(DEG):
            q = moved(pi)
            length = rho_k / pick(q[0], k)
            less = -length
            change = pair_scale(q, less, split(less))
            rho = pair_add(rho, change)
            fresh = pick(rho[0], k + 1)
            ratio = (-2.0 if k == 0 else -1.0) * length * (fresh / rho_k)
            pi = pair_add(rho, pair_scale(pi, ratio, split(ratio)))
            rho_k = fresh
            q_c = apply_b(p_c)
            x_c = x_c + (length * (2.0 / HALF)) * p_c
            r_c = r_c - length * q_c
            p_c = r_c + ratio * p_c

        lanes = list(range(DEG + 1)) + (list(range(BLOCK, BLOCK + DEG)) if two else [])
        xw, rw, pw = ([pick(c, lane) for lane in lanes] for c in (x_c, r_c, p_c))
        for z in range(bz):
            for h in range(halves):
                here = (HALO + z, h, mid_y, slice(None))
                vs = [ref[here] for ref in p_at] + [p_high[k, z, h] for k in range(HALO)]
                if two:
                    vs += [ref[here] for ref in r_at] + [r_high[k, z, h] for k in range(HALO - 1)]

                def mix(w):
                    out = w[0] * vs[0]
                    for a, b in zip(w[1:], vs[1:]):
                        out = out + a * b
                    return out
                total[0, z, h] = total[0, z, h] + mix(xw)
                fields[RES, HALO + z, h, mid_y, :] = mix(rw)
                fields[DIR, HALO + z, h, mid_y, :] = mix(pw)

    outer(0, False)

    def later(t, carry):
        exchange(((DIR, HALO, 0), (RES, HALO, 1)))
        outer(t, True)
        return carry
    lax.fori_loop(1, ROUNDS, later, 0)

    total[1] = fields[RES, mid_z, :, mid_y, :]
    copies = []
    for k, out in enumerate((sol_out, res_out)):
        copies.append(pltpu.make_async_remote_copy(
            src_ref=total.at[k, :, other], dst_ref=out.at[:, row_tile(ix), :],
            send_sem=swap_send.at[k], recv_sem=swap_recv.at[k],
            device_id=(iz, iy, other), device_id_type=MESH))
        copies.append(pltpu.make_async_copy(total.at[k, :, ix], out.at[:, row_tile(ix), :], own_sem.at[k]))
    for copy in copies:
        copy.start()
    for copy in copies:
        copy.wait()


def solution(mesh):
    nz, ny, nx = mesh.shape["gz"], mesh.shape["gy"], mesh.shape["gx"]

    def body(right_side, diagonal):
        bz, by, bx = right_side.shape
        hy = by // 2
        assert nx == 2 and bz >= HALO and hy == ROWS and bx == LANES
        ze, ye = bz + 2 * HALO, hy + 4 * ROWS
        f32, dma = jnp.float32, pltpu.SemaphoreType.DMA
        return pl.pallas_call(
            lambda *refs: kernel(nz, ny, nx, *refs),
            out_shape=(jax.ShapeDtypeStruct(right_side.shape, f32),) * 2,
            in_specs=[pl.BlockSpec(memory_space=pl.ANY)] * 2,
            out_specs=(pl.BlockSpec(memory_space=pl.ANY),) * 2,
            scratch_shapes=[
                pltpu.VMEM((5, ze, nx, ye, bx), f32),
                pltpu.VMEM((HALO - 1, ze, nx, ye, bx), f32),
                pltpu.VMEM((HALO - 1, ze, nx, ye, bx), f32),
                pltpu.VMEM((HALO, ze, nx, ye, bx), f32),
                pltpu.VMEM((HALO - 1, ze, nx, ye, bx), f32),
                pltpu.VMEM((HALO, bz, nx, hy, bx), f32),
                pltpu.VMEM((HALO - 1, bz, nx, hy, bx), f32),
                pltpu.VMEM((ze, nx, hy + 2 * ROWS, bx), f32),
                pltpu.VMEM((ze, 3, ROWS, bx), f32),
                pltpu.VMEM((2, bz, nx, hy, bx), f32),
                pltpu.VMEM((LANES, LANES), f32),
                pltpu.VMEM((1, LANES), f32),
                pltpu.VMEM((ROUNDS, ny * nx, 1, LANES), f32),
                pltpu.VMEM((1, LANES), f32),
                pltpu.VMEM((ROUNDS, nz, 1, LANES), f32),
                dma((4, 2)), dma((4, 2)), dma((4, 2, 3)), dma((4, 2, 3)),
                dma, dma((ROUNDS,)), dma, dma((ROUNDS,)),
                dma((2,)), dma((2,)), dma((2,)),
            ],
            compiler_params=pltpu.CompilerParams(collective_id=0, has_side_effects=True),
        )(right_side, diagonal)

    spec = P("gz", "gy", "gx")
    return jax.shard_map(body, mesh=mesh, in_specs=(spec, spec), out_specs=(spec, spec), check_vma=False)
```

```python
import jax
import jax.numpy as jnp
from jax import lax
from jax.experimental import pallas as pl
from jax.experimental.pallas import tpu as pltpu
from jax.sharding import PartitionSpec as P

S = 6
OUTER = 5
ROUNDS = 3
DEG = S * OUTER // ROUNDS
HALO = DEG // 2
SHIFT = 19.0
HALF = 19.0
LANES = 128
ROWS = 8
BLOCK = 64
MESH = pl.DeviceIdType.MESH


def two_sum(a, b):
    s = a + b
    t = s - a
    return s, (a - (s - t)) + (b - t)


def pair_add(a, b):
    s, e = two_sum(a[0], b[0])
    e = e + (a[1] + b[1])
    h = s + e
    return h, e - (h - s)


def split(a):
    c = 4097.0 * a
    high = c - (c - a)
    return high, a - high


def pair_scale(a, b, b_parts):
    p = a[0] * b
    h, l = split(a[0])
    e = ((h * b_parts[0] - p) + h * b_parts[1] + l * b_parts[0]) + l * b_parts[1]
    e = e + a[1] * b
    s = p + e
    return s, e - (s - p)


def kernel(nz, ny, nx, rhs_ref, diag_ref, sol_out, res_out,
           fields, p_low, r_low, p_wave, r_wave, p_high, r_high, scale2, weight, total, pairs,
           a_send, a_recv, b_send, b_recv,
           z_send, z_recv, y_send, y_recv, a_ssem, a_rsem, b_ssem, b_rsem, swap_send, swap_recv, own_sem):
    bz, by, bx = rhs_ref.shape
    hy = by // 2
    ze, halves, ya = fields.shape[1:4]
    first = (ya - hy) // 2
    low_rows, high_rows = slice(first - ROWS, first), slice(first + hy, first + hy + ROWS)
    iz, iy, ix = lax.axis_index("gz"), lax.axis_index("gy"), lax.axis_index("gx")
    other = 1 - ix
    yy = iy * 2 + ix
    has_z = (iz > 0, iz < nz - 1)
    has_y = (yy > 0, yy < 2 * ny - 1)
    z_dev = tuple((iz + s, iy, ix) for s in (-1, 1))
    y_dev = tuple((iz, (yy + s) // 2, other) for s in (-1, 1))
    mid_z, mid_y = slice(HALO, HALO + bz), slice(first, first + hy)
    RES, DIR, DIA, DIR5, RES5 = range(5)

    def row_tile(index):
        return pl.ds(pl.multiple_of(index * hy, hy), hy)

    barrier = pltpu.get_barrier_semaphore()
    for k in range(1, ny * nx):
        peer = (yy + k) % (ny * nx)
        pl.semaphore_signal(barrier, inc=1, device_id=(iz, peer // nx, peer % nx), device_id_type=MESH)
    for k in range(1, nz):
        pl.semaphore_signal(barrier, inc=1, device_id=((iz + k) % nz, iy, ix), device_id_type=MESH)

    owns = []
    spots = [(ref, fields.at[field, mid_z, ix, mid_y, :]) for ref, field in ((rhs_ref, DIR), (diag_ref, DIA))]
    for k, (ref, spot) in enumerate(spots):
        own = pltpu.make_async_copy(ref.at[:, row_tile(ix), :], spot, own_sem.at[k])
        own.start()
        owns.append(own)

    for side in range(2):
        planes = slice(0, HALO) if side == 0 else slice(HALO + bz, ze)
        rows = (low_rows, high_rows)[side]

        @pl.when(jnp.logical_not(has_z[side]))
        def _():
            for k in range(5):
                fields[k, planes] = jnp.zeros((HALO, halves, ya, bx), jnp.float32)

        @pl.when(jnp.logical_not(has_y[side]))
        def _():
            for k in range(5):
                fields[k, :, :, rows, :] = jnp.zeros((ze, halves, ROWS, bx), jnp.float32)

    w_unit = 2.0 / HALF
    w_low = jnp.where(has_y[0], jnp.float32(w_unit), 0.0)
    w_high = jnp.where(has_y[1], jnp.float32(w_unit), 0.0)
    z_low = jnp.where(has_z[0], jnp.float32(1.0), 0.0)
    z_high = jnp.where(has_z[1], jnp.float32(1.0), 0.0)
    for plane in range(ze):
        factor = z_low if plane < HALO else (z_high if plane >= HALO + bz else jnp.float32(1.0))
        for tile, w in enumerate((w_low, jnp.float32(w_unit), w_high)):
            weight[plane, tile] = jnp.broadcast_to(w * factor, (ROWS, bx))
    total[...] = jnp.zeros(total.shape, jnp.float32)
    pairs[...] = jnp.zeros(pairs.shape, jnp.float32)

    pl.semaphore_wait(barrier, ny * nx - 1 + nz - 1)
    swaps = []
    for k, (ref, spot) in enumerate(spots):
        swap = pltpu.make_async_remote_copy(
            src_ref=ref.at[:, row_tile(other), :], dst_ref=spot,
            send_sem=swap_send.at[k], recv_sem=swap_recv.at[k],
            device_id=(iz, iy, other), device_id_type=MESH)
        swap.start()
        swaps.append(swap)
    for copy in owns + swaps:
        copy.wait()

    def z_copy(item, side):
        field, depth, k = item
        low_src, high_src = slice(HALO, HALO + depth), slice(HALO + bz - depth, HALO + bz)
        low_dst, high_dst = slice(HALO - depth, HALO), slice(HALO + bz, HALO + bz + depth)
        src, dst = ((low_src, high_dst), (high_src, low_dst))[side]
        return pltpu.make_async_remote_copy(
            src_ref=fields.at[field, src, :, mid_y, :], dst_ref=fields.at[field, dst, :, mid_y, :],
            send_sem=z_send.at[k, side], recv_sem=z_recv.at[k, 1 - side],
            device_id=z_dev[side], device_id_type=MESH)

    def y_copy(item, side, part):
        field, depth, k = item
        planes = (mid_z, slice(HALO - depth, HALO), slice(HALO + bz, HALO + bz + depth))[part]
        low_src, high_src = slice(first, first + depth), slice(first + hy - depth, first + hy)
        low_dst, high_dst = slice(first - depth, first), slice(first + hy, first + hy + depth)
        src, dst = ((low_src, high_dst), (high_src, low_dst))[side]
        return pltpu.make_async_remote_copy(
            src_ref=fields.at[field, planes, :, src, :], dst_ref=fields.at[field, planes, :, dst, :],
            send_sem=y_send.at[k, side, part], recv_sem=y_recv.at[k, 1 - side, part],
            device_id=y_dev[side], device_id_type=MESH)

    def exchange(items):
        for item in items:
            for side in range(2):
                @pl.when(has_z[side])
                def _():
                    z_copy(item, side).start()
        for item in items:
            for side in range(2):
                @pl.when(has_y[side])
                def _():
                    y_copy(item, side, 0).start()
        for item in items:
            for z_side in range(2):
                @pl.when(has_z[z_side])
                def _():
                    z_copy(item, 1 - z_side).wait_recv()
                    for side in range(2):
                        @pl.when(has_y[side])
                        def _():
                            y_copy(item, side, 1 + z_side).start()
        for item in items:
            for side in range(2):
                @pl.when(has_z[side])
                def _():
                    z_copy(item, side).wait_send()

                @pl.when(has_y[side])
                def _():
                    y_copy(item, side, 0).wait_send()
                    y_copy(item, 1 - side, 0).wait_recv()
                    for z_side in range(2):
                        @pl.when(has_z[z_side])
                        def _():
                            y_copy(item, side, 1 + z_side).wait_send()
                            y_copy(item, 1 - side, 1 + z_side).wait_recv()

    exchange(((DIR, HALO, 0), (DIA, HALO - 1, 1)))
    all_rows = slice(first - ROWS, first + hy + ROWS)

    def prepare(plane, c):
        scale2[plane] = (fields[DIA, plane, :, all_rows, :] + (27.0 - SHIFT)) * (2.0 / HALF)
        return c
    lax.fori_loop(0, ze, prepare, 0)

    tiles = (hy + 2 * ROWS) // ROWS
    lane_id = lax.broadcasted_iota(jnp.int32, (ROWS, bx), 1)
    first_lane, last_lane = lane_id == 0, lane_id == bx - 1

    def row_sums(ref, z, tile):
        at = first - ROWS + tile * ROWS
        return [ref[z, h, at - 1:at - 1 + ROWS, :] + ref[z, h, at:at + ROWS, :] + ref[z, h, at + 1:at + 1 + ROWS, :]
                for h in range(halves)]

    def lane_sums(parts):
        left = [pltpu.roll(v, 1, 1) for v in parts]
        right = [pltpu.roll(v, bx - 1, 1) for v in parts]
        out = []
        for h in range(halves):
            before = left[h - 1] if h else 0.0
            after = right[h + 1] if h < halves - 1 else 0.0
            out.append(parts[h] + jnp.where(first_lane, before, left[h]) + jnp.where(last_lane, after, right[h]))
        return out

    p_at = [fields.at[DIR]] + [p_low.at[k] for k in range(HALO - 1)] + [fields.at[DIR5]]
    r_at = [fields.at[RES]] + [r_low.at[k] for k in range(HALO - 1)] + [fields.at[RES5]]
    p_on = [fields.at[DIR5]] + [p_wave.at[k] for k in range(HALO)]
    r_on = [fields.at[RES5]] + [r_wave.at[k] for k in range(HALO - 1)]

    def sweep(chain, degree, depth):
        start, stop = HALO - depth, HALO + bz + depth
        chosen = range(tiles) if depth else (1,)

        def step(z, carry):
            out = []
            for tile, (before, here) in zip(chosen, carry):
                after = row_sums(chain[degree], z + 1, tile)
                box = lane_sums([a + b + c for a, b, c in zip(before, here, after)])
                at = first - ROWS + tile * ROWS
                for h in range(halves):
                    value = (scale2[z, h, tile * ROWS:(tile + 1) * ROWS, :] * chain[degree][z, h, at:at + ROWS, :]
                             - weight[z, tile] * box[h])
                    if degree == 0:
                        value = 0.5 * value
                    else:
                        value = value - chain[degree - 1][z, h, at:at + ROWS, :]
                    chain[degree + 1][z, h, at:at + ROWS, :] = value
                out.append((here, after))
            return tuple(out)
        carry = tuple((row_sums(chain[degree], start - 1, k), row_sums(chain[degree], start, k)) for k in chosen)
        for z in range(start, stop):
            carry = step(z, carry)

    gl = lax.broadcasted_iota(jnp.int32, (ROWS, LANES), 1)
    zero_lane, up_twice = gl == 0, jnp.where((gl == 1) | (gl == BLOCK + 1), jnp.float32(2.0), jnp.float32(1.0))
    in_block = (gl <= DEG) | ((gl >= BLOCK) & (gl <= BLOCK + DEG))

    def pick(v, lane):
        return jnp.broadcast_to(v[:, lane:lane + 1], (ROWS, LANES))

    def moved(pair):
        up = [pltpu.roll(v, LANES - 1, 1) for v in pair]
        down = [jnp.where(zero_lane, u, pltpu.roll(v, 1, 1)) for u, v in zip(up, pair)]
        return pair_add((2.0 * pair[0], 2.0 * pair[1]), pair_add(up, down))

    def apply_b(c):
        return jnp.where(in_block, 2.0 * c + up_twice * pltpu.roll(c, 1, 1) + pltpu.roll(c, LANES - 1, 1), 0.0)

    def everywhere(row, slot):
        a_me, b_me = yy, iz
        a_count, b_count = ny * nx, nz

        def stage(send_ref, recv_ref, me, count, ssem, rsem, dev, value):
            send_ref[...] = value
            recv_ref[slot, me] = value
            for k in range(1, count):
                peer = (me + k) % count
                pltpu.make_async_remote_copy(
                    src_ref=send_ref, dst_ref=recv_ref.at[slot, me],
                    send_sem=ssem, recv_sem=rsem.at[slot],
                    device_id=dev(peer), device_id_type=MESH).start()
            most = recv_ref.at[slot, 0:count - 1]
            pltpu.make_async_copy(most, most, rsem.at[slot]).wait()
            out = jnp.sum(recv_ref[slot], axis=0)
            pltpu.make_async_copy(most, most, ssem).wait()
            return out
        mine = stage(a_send, a_recv, a_me, a_count, a_ssem, a_rsem, lambda p: (iz, p // nx, p % nx), row)
        return stage(b_send, b_recv, b_me, b_count, b_ssem, b_rsem, lambda p: (p, iy, ix), mine)

    def outer(t, two):
        for degree in range(HALO):
            sweep(p_at, degree, HALO - 1 - degree)
            if two:
                sweep(r_at, degree, HALO - 1 - degree)
        exchange(((DIR5, HALO, 2), (RES5, HALO - 1, 3)) if two else ((DIR5, HALO, 2),))
        for degree in range(HALO):
            sweep(p_on, degree, HALO - 1 - degree)
            if two and degree < HALO - 1:
                sweep(r_on, degree, HALO - 2 - degree)

        sums = {}

        def add(key, value):
            sums[key] = sums[key] + value if key in sums else value
        for z in range(bz):
            for h in range(halves):
                here = (HALO + z, h, mid_y, slice(None))
                lists = []
                for low, wave, high in ((p_at, p_on, p_high), (r_at, r_on, r_high))[:1 + two]:
                    vs = [ref[here] for ref in low]
                    for k in range(1, len(wave)):
                        value = 2.0 * wave[k][here] - vs[HALO - k]
                        high[k - 1, z, h] = value
                        vs.append(value)
                    lists.append(vs)
                ps = lists[0]
                for k in range(2 * DEG + 1):
                    add(k, ps[(k + 1) // 2] * ps[k // 2])
                if two:
                    rs = lists[1]
                    for k in range(2 * DEG):
                        add(BLOCK + k, ps[(k + 1) // 2] * rs[k // 2])
        lines = {}
        for key, value in sums.items():
            base = key // BLOCK * BLOCK
            if key - base > 1:
                value = 2.0 * value - sums[base + (key - base) % 2]
            pairs[key:key + 1, :] = jnp.sum(value, axis=0, keepdims=True)
        row = jnp.sum(pairs[...].T, axis=0, keepdims=True)
        row = jnp.broadcast_to(everywhere(row, t), (ROWS, LANES))

        nil = jnp.zeros((ROWS, LANES), jnp.float32)
        pi = (row, nil)
        rho = (pltpu.roll(row, LANES - BLOCK, 1), nil) if two else pi
        p_c = (gl == 0).astype(jnp.float32)
        r_c = (gl == BLOCK).astype(jnp.float32) if two else p_c
        x_c = nil
        q = moved(pi)
        rho_k = pick(rho[0], 0)
        for k in range(DEG):
            inverse = 1.0 / pick(q[0], k)
            length = rho_k * inverse
            less = -length
            rho = pair_add(rho, pair_scale(q, less, split(less)))
            fresh = pick(rho[0], k + 1)
            ratio = ((-2.0 if k == 0 else -1.0) * inverse) * fresh
            if k < DEG - 1:
                q = pair_add(moved(rho), pair_scale(q, ratio, split(ratio)))
            rho_k = fresh
            q_c = apply_b(p_c)
            x_c = x_c + (length * (2.0 / HALF)) * p_c
            r_c = r_c - length * q_c
            p_c = r_c + ratio * p_c

        lanes = list(range(DEG + 1)) + (list(range(BLOCK, BLOCK + DEG)) if two else [])
        xw, rw, pw = ([pick(c, lane) for lane in lanes] for c in (x_c, r_c, p_c))
        for z in range(bz):
            for h in range(halves):
                here = (HALO + z, h, mid_y, slice(None))
                vs = [ref[here] for ref in p_at] + [p_high[k, z, h] for k in range(HALO)]
                if two:
                    vs += [ref[here] for ref in r_at] + [r_high[k, z, h] for k in range(HALO - 1)]

                def mix(w):
                    out = w[0] * vs[0]
                    for a, b in zip(w[1:], vs[1:]):
                        out = out + a * b
                    return out
                total[0, z, h] = total[0, z, h] + mix(xw)
                fields[RES, HALO + z, h, mid_y, :] = mix(rw)
                fields[DIR, HALO + z, h, mid_y, :] = mix(pw)

    outer(0, False)

    def later(t, carry):
        exchange(((DIR, HALO, 0), (RES, HALO, 1)))
        outer(t, True)
        return carry
    lax.fori_loop(1, ROUNDS, later, 0)

    total[1] = fields[RES, mid_z, :, mid_y, :]
    copies = []
    for k, out in enumerate((sol_out, res_out)):
        copies.append(pltpu.make_async_remote_copy(
            src_ref=total.at[k, :, other], dst_ref=out.at[:, row_tile(ix), :],
            send_sem=swap_send.at[k], recv_sem=swap_recv.at[k],
            device_id=(iz, iy, other), device_id_type=MESH))
        copies.append(pltpu.make_async_copy(total.at[k, :, ix], out.at[:, row_tile(ix), :], own_sem.at[k]))
    for copy in copies:
        copy.start()
    for copy in copies:
        copy.wait()


def solution(mesh):
    nz, ny, nx = mesh.shape["gz"], mesh.shape["gy"], mesh.shape["gx"]

    def body(right_side, diagonal):
        bz, by, bx = right_side.shape
        hy = by // 2
        assert nx == 2 and bz >= HALO and hy == ROWS and bx == LANES
        ze, ye = bz + 2 * HALO, hy + 4 * ROWS
        f32, dma = jnp.float32, pltpu.SemaphoreType.DMA
        return pl.pallas_call(
            lambda *refs: kernel(nz, ny, nx, *refs),
            out_shape=(jax.ShapeDtypeStruct(right_side.shape, f32),) * 2,
            in_specs=[pl.BlockSpec(memory_space=pl.ANY)] * 2,
            out_specs=(pl.BlockSpec(memory_space=pl.ANY),) * 2,
            scratch_shapes=[
                pltpu.VMEM((5, ze, nx, ye, bx), f32),
                pltpu.VMEM((HALO - 1, ze, nx, ye, bx), f32),
                pltpu.VMEM((HALO - 1, ze, nx, ye, bx), f32),
                pltpu.VMEM((HALO, ze, nx, ye, bx), f32),
                pltpu.VMEM((HALO - 1, ze, nx, ye, bx), f32),
                pltpu.VMEM((HALO, bz, nx, hy, bx), f32),
                pltpu.VMEM((HALO - 1, bz, nx, hy, bx), f32),
                pltpu.VMEM((ze, nx, hy + 2 * ROWS, bx), f32),
                pltpu.VMEM((ze, 3, ROWS, bx), f32),
                pltpu.VMEM((2, bz, nx, hy, bx), f32),
                pltpu.VMEM((LANES, LANES), f32),
                pltpu.VMEM((1, LANES), f32),
                pltpu.VMEM((ROUNDS, ny * nx, 1, LANES), f32),
                pltpu.VMEM((1, LANES), f32),
                pltpu.VMEM((ROUNDS, nz, 1, LANES), f32),
                dma((4, 2)), dma((4, 2)), dma((4, 2, 3)), dma((4, 2, 3)),
                dma, dma((ROUNDS,)), dma, dma((ROUNDS,)),
                dma((2,)), dma((2,)), dma((2,)),
            ],
            compiler_params=pltpu.CompilerParams(collective_id=0, has_side_effects=True),
        )(right_side, diagonal)

    spec = P("gz", "gy", "gx")
    return jax.shard_map(body, mesh=mesh, in_specs=(spec, spec), out_specs=(spec, spec), check_vma=False)
```

```python
import jax
import jax.numpy as jnp
from jax import lax
from jax.experimental import pallas as pl
from jax.experimental.pallas import tpu as pltpu
from jax.sharding import PartitionSpec as P

S = 6
OUTER = 5
ROUNDS = 3
DEG = S * OUTER // ROUNDS
HALO = DEG // 2
SHIFT = 19.0
HALF = 19.0
LANES = 128
ROWS = 8
BLOCK = 64
MESH = pl.DeviceIdType.MESH


def two_sum(a, b):
    s = a + b
    t = s - a
    return s, (a - (s - t)) + (b - t)


def pair_add(a, b):
    s, e = two_sum(a[0], b[0])
    e = e + (a[1] + b[1])
    h = s + e
    return h, e - (h - s)


def split(a):
    c = 4097.0 * a
    high = c - (c - a)
    return high, a - high


def pair_scale(a, b, b_parts):
    p = a[0] * b
    h, l = split(a[0])
    e = ((h * b_parts[0] - p) + h * b_parts[1] + l * b_parts[0]) + l * b_parts[1]
    e = e + a[1] * b
    s = p + e
    return s, e - (s - p)


def kernel(nz, ny, nx, rhs_ref, diag_ref, sol_out, res_out,
           fields, p_low, r_low, p_wave, r_wave, p_high, r_high, scale2, weight, total, pairs,
           a_send, a_recv, b_send, b_recv,
           z_send, z_recv, y_send, y_recv, a_ssem, a_rsem, b_ssem, b_rsem, swap_send, swap_recv, own_sem):
    bz, by, bx = rhs_ref.shape
    hy = by // 2
    ze, halves, ya = fields.shape[1:4]
    first = (ya - hy) // 2
    low_rows, high_rows = slice(first - ROWS, first), slice(first + hy, first + hy + ROWS)
    iz, iy, ix = lax.axis_index("gz"), lax.axis_index("gy"), lax.axis_index("gx")
    other = 1 - ix
    yy = iy * 2 + ix
    has_z = (iz > 0, iz < nz - 1)
    has_y = (yy > 0, yy < 2 * ny - 1)
    z_dev = tuple((iz + s, iy, ix) for s in (-1, 1))
    y_dev = tuple((iz, (yy + s) // 2, other) for s in (-1, 1))
    mid_z, mid_y = slice(HALO, HALO + bz), slice(first, first + hy)
    RES, DIR, DIA, DIR5, RES5 = range(5)

    def row_tile(index):
        return pl.ds(pl.multiple_of(index * hy, hy), hy)

    barrier = pltpu.get_barrier_semaphore()
    for k in range(1, ny * nx):
        peer = (yy + k) % (ny * nx)
        pl.semaphore_signal(barrier, inc=1, device_id=(iz, peer // nx, peer % nx), device_id_type=MESH)
    for k in range(1, nz):
        pl.semaphore_signal(barrier, inc=1, device_id=((iz + k) % nz, iy, ix), device_id_type=MESH)

    owns = []
    spots = [(ref, fields.at[field, mid_z, ix, mid_y, :]) for ref, field in ((rhs_ref, DIR), (diag_ref, DIA))]
    for k, (ref, spot) in enumerate(spots):
        own = pltpu.make_async_copy(ref.at[:, row_tile(ix), :], spot, own_sem.at[k])
        own.start()
        owns.append(own)

    for side in range(2):
        planes = slice(0, HALO) if side == 0 else slice(HALO + bz, ze)
        rows = (low_rows, high_rows)[side]

        @pl.when(jnp.logical_not(has_z[side]))
        def _():
            for k in range(5):
                fields[k, planes] = jnp.zeros((HALO, halves, ya, bx), jnp.float32)

        @pl.when(jnp.logical_not(has_y[side]))
        def _():
            for k in range(5):
                fields[k, :, :, rows, :] = jnp.zeros((ze, halves, ROWS, bx), jnp.float32)

    w_unit = 2.0 / HALF
    w_low = jnp.where(has_y[0], jnp.float32(w_unit), 0.0)
    w_high = jnp.where(has_y[1], jnp.float32(w_unit), 0.0)
    z_low = jnp.where(has_z[0], jnp.float32(1.0), 0.0)
    z_high = jnp.where(has_z[1], jnp.float32(1.0), 0.0)
    for plane in range(ze):
        factor = z_low if plane < HALO else (z_high if plane >= HALO + bz else jnp.float32(1.0))
        for tile, w in enumerate((w_low, jnp.float32(w_unit), w_high)):
            weight[plane, tile] = jnp.broadcast_to(w * factor, (ROWS, bx))
    total[...] = jnp.zeros(total.shape, jnp.float32)
    pairs[...] = jnp.zeros(pairs.shape, jnp.float32)

    pl.semaphore_wait(barrier, ny * nx - 1 + nz - 1)
    swaps = []
    for k, (ref, spot) in enumerate(spots):
        swap = pltpu.make_async_remote_copy(
            src_ref=ref.at[:, row_tile(other), :], dst_ref=spot,
            send_sem=swap_send.at[k], recv_sem=swap_recv.at[k],
            device_id=(iz, iy, other), device_id_type=MESH)
        swap.start()
        swaps.append(swap)
    for copy in owns + swaps:
        copy.wait()

    def z_copy(item, side):
        field, depth, k = item
        low_src, high_src = slice(HALO, HALO + depth), slice(HALO + bz - depth, HALO + bz)
        low_dst, high_dst = slice(HALO - depth, HALO), slice(HALO + bz, HALO + bz + depth)
        src, dst = ((low_src, high_dst), (high_src, low_dst))[side]
        return pltpu.make_async_remote_copy(
            src_ref=fields.at[field, src, :, mid_y, :], dst_ref=fields.at[field, dst, :, mid_y, :],
            send_sem=z_send.at[k, side], recv_sem=z_recv.at[k, 1 - side],
            device_id=z_dev[side], device_id_type=MESH)

    def y_copy(item, side, part):
        field, depth, k = item
        planes = (mid_z, slice(HALO - depth, HALO), slice(HALO + bz, HALO + bz + depth))[part]
        low_src, high_src = slice(first, first + depth), slice(first + hy - depth, first + hy)
        low_dst, high_dst = slice(first - depth, first), slice(first + hy, first + hy + depth)
        src, dst = ((low_src, high_dst), (high_src, low_dst))[side]
        return pltpu.make_async_remote_copy(
            src_ref=fields.at[field, planes, :, src, :], dst_ref=fields.at[field, planes, :, dst, :],
            send_sem=y_send.at[k, side, part], recv_sem=y_recv.at[k, 1 - side, part],
            device_id=y_dev[side], device_id_type=MESH)

    def exchange(items):
        for item in items:
            for side in range(2):
                @pl.when(has_z[side])
                def _():
                    z_copy(item, side).start()
        for item in items:
            for side in range(2):
                @pl.when(has_y[side])
                def _():
                    y_copy(item, side, 0).start()
        for item in items:
            for z_side in range(2):
                @pl.when(has_z[z_side])
                def _():
                    z_copy(item, 1 - z_side).wait_recv()
                    for side in range(2):
                        @pl.when(has_y[side])
                        def _():
                            y_copy(item, side, 1 + z_side).start()
        for item in items:
            for side in range(2):
                @pl.when(has_z[side])
                def _():
                    z_copy(item, side).wait_send()

                @pl.when(has_y[side])
                def _():
                    y_copy(item, side, 0).wait_send()
                    y_copy(item, 1 - side, 0).wait_recv()
                    for z_side in range(2):
                        @pl.when(has_z[z_side])
                        def _():
                            y_copy(item, side, 1 + z_side).wait_send()
                            y_copy(item, 1 - side, 1 + z_side).wait_recv()

    exchange(((DIR, HALO, 0), (DIA, HALO - 1, 1)))
    all_rows = slice(first - ROWS, first + hy + ROWS)

    def prepare(plane, c):
        scale2[plane] = (fields[DIA, plane, :, all_rows, :] + (27.0 - SHIFT)) * (2.0 / HALF)
        return c
    lax.fori_loop(0, ze, prepare, 0)

    tiles = (hy + 2 * ROWS) // ROWS
    lane_id = lax.broadcasted_iota(jnp.int32, (ROWS, bx), 1)
    first_lane, last_lane = lane_id == 0, lane_id == bx - 1

    def row_sums(ref, z, tile):
        at = first - ROWS + tile * ROWS
        return [ref[z, h, at - 1:at - 1 + ROWS, :] + ref[z, h, at:at + ROWS, :] + ref[z, h, at + 1:at + 1 + ROWS, :]
                for h in range(halves)]

    def lane_sums(parts):
        left = [pltpu.roll(v, 1, 1) for v in parts]
        right = [pltpu.roll(v, bx - 1, 1) for v in parts]
        out = []
        for h in range(halves):
            before = left[h - 1] if h else 0.0
            after = right[h + 1] if h < halves - 1 else 0.0
            out.append(parts[h] + jnp.where(first_lane, before, left[h]) + jnp.where(last_lane, after, right[h]))
        return out

    p_at = [fields.at[DIR]] + [p_low.at[k] for k in range(HALO - 1)] + [fields.at[DIR5]]
    r_at = [fields.at[RES]] + [r_low.at[k] for k in range(HALO - 1)] + [fields.at[RES5]]
    p_on = [fields.at[DIR5]] + [p_wave.at[k] for k in range(HALO)]
    r_on = [fields.at[RES5]] + [r_wave.at[k] for k in range(HALO - 1)]

    def sweep(chain, degree, depth):
        start, stop = HALO - depth, HALO + bz + depth
        chosen = range(tiles) if depth else (1,)

        def step(z, carry):
            out = []
            for tile, (before, here) in zip(chosen, carry):
                after = row_sums(chain[degree], z + 1, tile)
                box = lane_sums([a + b + c for a, b, c in zip(before, here, after)])
                at = first - ROWS + tile * ROWS
                for h in range(halves):
                    value = (scale2[z, h, tile * ROWS:(tile + 1) * ROWS, :] * chain[degree][z, h, at:at + ROWS, :]
                             - weight[z, tile] * box[h])
                    if degree == 0:
                        value = 0.5 * value
                    else:
                        value = value - chain[degree - 1][z, h, at:at + ROWS, :]
                    chain[degree + 1][z, h, at:at + ROWS, :] = value
                out.append((here, after))
            return tuple(out)
        carry = tuple((row_sums(chain[degree], start - 1, k), row_sums(chain[degree], start, k)) for k in chosen)
        for z in range(start, stop):
            carry = step(z, carry)

    gl = lax.broadcasted_iota(jnp.int32, (ROWS, LANES), 1)
    zero_lane, up_twice = gl == 0, jnp.where((gl == 1) | (gl == BLOCK + 1), jnp.float32(2.0), jnp.float32(1.0))
    in_block = (gl <= DEG) | ((gl >= BLOCK) & (gl <= BLOCK + DEG))

    def pick(v, lane):
        return jnp.broadcast_to(v[:, lane:lane + 1], (ROWS, LANES))

    def moved(pair):
        up = [pltpu.roll(v, LANES - 1, 1) for v in pair]
        down = [jnp.where(zero_lane, u, pltpu.roll(v, 1, 1)) for u, v in zip(up, pair)]
        return pair_add((2.0 * pair[0], 2.0 * pair[1]), pair_add(up, down))

    def apply_b(c):
        return jnp.where(in_block, 2.0 * c + up_twice * pltpu.roll(c, 1, 1) + pltpu.roll(c, LANES - 1, 1), 0.0)

    def everywhere(row, slot):
        a_me, b_me = yy, iz
        a_count, b_count = ny * nx, nz

        def stage(send_ref, recv_ref, me, count, ssem, rsem, dev, value):
            send_ref[...] = value
            recv_ref[slot, me] = value
            for k in sorted(range(1, count), key=lambda k: -min(k % 8, 8 - k % 8) - 2 * min(k // 8, (count - k) // 8)):
                peer = (me + k) % count
                pltpu.make_async_remote_copy(
                    src_ref=send_ref, dst_ref=recv_ref.at[slot, me],
                    send_sem=ssem, recv_sem=rsem.at[slot],
                    device_id=dev(peer), device_id_type=MESH).start()
            most = recv_ref.at[slot, 0:count - 1]
            pltpu.make_async_copy(most, most, rsem.at[slot]).wait()
            return jnp.sum(recv_ref[slot], axis=0)
        mine = stage(a_send, a_recv, a_me, a_count, a_ssem, a_rsem, lambda p: (iz, p // nx, p % nx), row)
        out = stage(b_send, b_recv, b_me, b_count, b_ssem, b_rsem, lambda p: (p, iy, ix), mine)
        for recv_ref, count, ssem in ((a_recv, a_count, a_ssem), (b_recv, b_count, b_ssem)):
            most = recv_ref.at[slot, 0:count - 1]
            pltpu.make_async_copy(most, most, ssem).wait()
        return out

    def outer(t, two):
        for degree in range(HALO):
            sweep(p_at, degree, HALO - 1 - degree)
            if two:
                sweep(r_at, degree, HALO - 1 - degree)
        exchange(((DIR5, HALO, 2), (RES5, HALO - 1, 3)) if two else ((DIR5, HALO, 2),))
        for degree in range(HALO):
            sweep(p_on, degree, HALO - 1 - degree)
            if two and degree < HALO - 1:
                sweep(r_on, degree, HALO - 2 - degree)

        sums = {}

        def add(key, value):
            sums[key] = sums[key] + value if key in sums else value
        for z in range(bz):
            for h in range(halves):
                here = (HALO + z, h, mid_y, slice(None))
                lists = []
                for low, wave, high in ((p_at, p_on, p_high), (r_at, r_on, r_high))[:1 + two]:
                    vs = [ref[here] for ref in low]
                    for k in range(1, len(wave)):
                        value = 2.0 * wave[k][here] - vs[HALO - k]
                        high[k - 1, z, h] = value
                        vs.append(value)
                    lists.append(vs)
                ps = lists[0]
                for k in range(2 * DEG + 1):
                    add(k, ps[(k + 1) // 2] * ps[k // 2])
                if two:
                    rs = lists[1]
                    for k in range(2 * DEG):
                        add(BLOCK + k, ps[(k + 1) // 2] * rs[k // 2])
        lines = {}
        for key, value in sums.items():
            base = key // BLOCK * BLOCK
            if key - base > 1:
                value = 2.0 * value - sums[base + (key - base) % 2]
            pairs[key:key + 1, :] = jnp.sum(value, axis=0, keepdims=True)
        row = jnp.sum(pairs[...].T, axis=0, keepdims=True)
        row = jnp.broadcast_to(everywhere(row, t), (ROWS, LANES))

        nil = jnp.zeros((ROWS, LANES), jnp.float32)
        pi = (row, nil)
        rho = (pltpu.roll(row, LANES - BLOCK, 1), nil) if two else pi
        p_c = (gl == 0).astype(jnp.float32)
        r_c = (gl == BLOCK).astype(jnp.float32) if two else p_c
        x_c = nil
        q = moved(pi)
        rho_k = pick(rho[0], 0)
        for k in range(DEG):
            inverse = 1.0 / pick(q[0], k)
            length = rho_k * inverse
            less = -length
            rho = pair_add(rho, pair_scale(q, less, split(less)))
            fresh = pick(rho[0], k + 1)
            ratio = ((-2.0 if k == 0 else -1.0) * inverse) * fresh
            if k < DEG - 1:
                q = pair_add(moved(rho), pair_scale(q, ratio, split(ratio)))
            rho_k = fresh
            q_c = apply_b(p_c)
            x_c = x_c + (length * (2.0 / HALF)) * p_c
            r_c = r_c - length * q_c
            p_c = r_c + ratio * p_c

        lanes = list(range(DEG + 1)) + (list(range(BLOCK, BLOCK + DEG)) if two else [])
        xw, rw, pw = ([pick(c, lane) for lane in lanes] for c in (x_c, r_c, p_c))
        for z in range(bz):
            for h in range(halves):
                here = (HALO + z, h, mid_y, slice(None))
                vs = [ref[here] for ref in p_at] + [p_high[k, z, h] for k in range(HALO)]
                if two:
                    vs += [ref[here] for ref in r_at] + [r_high[k, z, h] for k in range(HALO - 1)]

                def mix(w):
                    out = w[0] * vs[0]
                    for a, b in zip(w[1:], vs[1:]):
                        out = out + a * b
                    return out
                total[0, z, h] = total[0, z, h] + mix(xw)
                fields[RES, HALO + z, h, mid_y, :] = mix(rw)
                fields[DIR, HALO + z, h, mid_y, :] = mix(pw)

    outer(0, False)

    def later(t, carry):
        exchange(((DIR, HALO, 0), (RES, HALO, 1)))
        outer(t, True)
        return carry
    lax.fori_loop(1, ROUNDS, later, 0)

    total[1] = fields[RES, mid_z, :, mid_y, :]
    copies = []
    for k, out in enumerate((sol_out, res_out)):
        copies.append(pltpu.make_async_remote_copy(
            src_ref=total.at[k, :, other], dst_ref=out.at[:, row_tile(ix), :],
            send_sem=swap_send.at[k], recv_sem=swap_recv.at[k],
            device_id=(iz, iy, other), device_id_type=MESH))
        copies.append(pltpu.make_async_copy(total.at[k, :, ix], out.at[:, row_tile(ix), :], own_sem.at[k]))
    for copy in copies:
        copy.start()
    for copy in copies:
        copy.wait()


def solution(mesh):
    nz, ny, nx = mesh.shape["gz"], mesh.shape["gy"], mesh.shape["gx"]

    def body(right_side, diagonal):
        bz, by, bx = right_side.shape
        hy = by // 2
        assert nx == 2 and bz >= HALO and hy == ROWS and bx == LANES
        ze, ye = bz + 2 * HALO, hy + 4 * ROWS
        f32, dma = jnp.float32, pltpu.SemaphoreType.DMA
        return pl.pallas_call(
            lambda *refs: kernel(nz, ny, nx, *refs),
            out_shape=(jax.ShapeDtypeStruct(right_side.shape, f32),) * 2,
            in_specs=[pl.BlockSpec(memory_space=pl.ANY)] * 2,
            out_specs=(pl.BlockSpec(memory_space=pl.ANY),) * 2,
            scratch_shapes=[
                pltpu.VMEM((5, ze, nx, ye, bx), f32),
                pltpu.VMEM((HALO - 1, ze, nx, ye, bx), f32),
                pltpu.VMEM((HALO - 1, ze, nx, ye, bx), f32),
                pltpu.VMEM((HALO, ze, nx, ye, bx), f32),
                pltpu.VMEM((HALO - 1, ze, nx, ye, bx), f32),
                pltpu.VMEM((HALO, bz, nx, hy, bx), f32),
                pltpu.VMEM((HALO - 1, bz, nx, hy, bx), f32),
                pltpu.VMEM((ze, nx, hy + 2 * ROWS, bx), f32),
                pltpu.VMEM((ze, 3, ROWS, bx), f32),
                pltpu.VMEM((2, bz, nx, hy, bx), f32),
                pltpu.VMEM((LANES, LANES), f32),
                pltpu.VMEM((1, LANES), f32),
                pltpu.VMEM((ROUNDS, ny * nx, 1, LANES), f32),
                pltpu.VMEM((1, LANES), f32),
                pltpu.VMEM((ROUNDS, nz, 1, LANES), f32),
                dma((4, 2)), dma((4, 2)), dma((4, 2, 3)), dma((4, 2, 3)),
                dma, dma((ROUNDS,)), dma, dma((ROUNDS,)),
                dma((2,)), dma((2,)), dma((2,)),
            ],
            compiler_params=pltpu.CompilerParams(collective_id=0, has_side_effects=True),
        )(right_side, diagonal)

    spec = P("gz", "gy", "gx")
    return jax.shard_map(body, mesh=mesh, in_specs=(spec, spec), out_specs=(spec, spec), check_vma=False)
```
